512 devices in a mesh: seq: 64 (over z, x, core), width: 8 (over y).
Axes of the slice: x: 4, y: 8, z: 8, core: 2. Of those that a mesh axis runs over, the one named last changes fastest.
Arguments:
- fade_rate: float32 [2, 32768, 2048], P(None, 'seq', 'width'), may hold values from 0.2 to 2
- update_in: bfloat16 [2, 32768, 2048], P(None, 'seq', 'width'), may hold values from -6 to 6
- gate_in: bfloat16 [2, 32768, 2048], P(None, 'seq', 'width'), may hold values from -6 to 6
Outputs:
- filtered: bfloat16 [2, 32768, 2048], P(None, 'seq', 'width')
The draws below stay inside these ranges and needn't reach their ends.
All inputs are finite; a program needn't handle non-finite values.
Results may differ from the reference program's by a relative error of at most 0.0015.
Values sent between devices are 32-bit elements; how exact they have to be, the bound alone decides.
A program may use at most 64 MiB of HBM per device.

```python
import jax
import jax.numpy as jnp
from jax import lax

BATCH = 2
CHANNELS = 2048
LENGTH = 32768


def level_of(key, dims, pieces, smallest, high):
    loudness, own = 1.0, jax.random.fold_in(key, 6)
    for dim, parts in pieces:
        draws = jnp.exp(jax.random.uniform(jax.random.fold_in(own, dim), (parts,), jnp.float32, smallest / len(pieces), high / len(pieces)))
        loudness = loudness * jnp.repeat(draws, dims[dim] // parts).reshape([-1 if axis == dim else 1 for axis in range(len(dims))])
    return loudness


def noise(own_key, dims, scale, reach, cuts=(), kind=jnp.bfloat16):
    factor_of = level_of(own_key, dims, cuts, -0.22, 0.18) if cuts else 1.0
    result = jax.random.normal(own_key, dims, jnp.float32) * scale * factor_of
    return jnp.minimum(jnp.maximum(result, -reach), reach).astype(kind)


def setup_inputs(seed: int = 0) -> dict:
    splits = jax.random.split(jax.random.key(seed), 4)
    return {
        "fade_rate": jnp.clip(0.2 + 1.8 * jax.random.uniform(splits[0], (BATCH, LENGTH, CHANNELS), jnp.float32) ** level_of(splits[0], (BATCH, LENGTH, CHANNELS), ((1, 64), (2, 8)), -0.2, 0.2), 0.2, 2.0),
        "update_in": noise(splits[1], (BATCH, LENGTH, CHANNELS), 1.0, 6.0, ((1, 64), (2, 8))),
        "gate_in": noise(splits[2], (BATCH, LENGTH, CHANNELS), 1.0, 6.0, ((1, 64), (2, 8))),
    }


def join_pair(earlier, later):
    return earlier[0] * later[0], later[0] * earlier[1] + later[1]


def reference(fade_rate, update_in, gate_in):
    keep = jnp.exp(-fade_rate / LENGTH)
    push = update_in.astype(jnp.float32) * LENGTH ** -0.5
    forward = lax.associative_scan(join_pair, (keep, push), axis=1)[1]
    backward = lax.associative_scan(join_pair, (keep, push), axis=1, reverse=True)[1]
    states = forward + backward
    gated = states * jax.nn.silu(gate_in.astype(jnp.float32))
    filtered = gated.astype(jnp.bfloat16)
    return filtered
```

```python
import functools

import jax
import jax.numpy as jnp
from jax import lax
from jax.experimental import pallas as pl
from jax.experimental.pallas import tpu as pltpu
from jax.sharding import PartitionSpec as P

MESH = pl.DeviceIdType.MESH
INNER = 8
LANES = 128


def triangle(rows, upper):
    r = lax.broadcasted_iota(jnp.int32, (rows, rows), 0)
    c = lax.broadcasted_iota(jnp.int32, (rows, rows), 1)
    inside = c >= r if upper else c <= r
    return jnp.where(inside, 1.0, 0.0).astype(jnp.bfloat16)


def running(mask, value):
    high = value.astype(jnp.bfloat16)
    low = (value - high.astype(jnp.float32)).astype(jnp.bfloat16)
    dot = functools.partial(jnp.dot, preferred_element_type=jnp.float32)
    return dot(mask, high) + dot(mask, low)


def kernel(
    outer, total_length, rows,
    fade_h, upd_h, gate_h, out_ref,
    fade_v, upd_v, gate_v, lower, upper, logs, base, qv, rv,
    row_out, row_in, far_out, far_in,
    load_sem, row_send, row_recv, far_send, far_recv,
):
    batch, length, width = fade_v.shape
    parts = length // rows
    tiles = width // LANES
    quantity = batch * tiles
    seq = lax.axis_index("seq")
    z, r = seq // INNER, seq % INNER

    def row_peer(d):
        return (r + d) % INNER

    def far_peer(d):
        return (z + d) % outer

    def order(count):
        return sorted(range(1, count), key=lambda d: -min(d, count - d))

    barrier = pltpu.get_barrier_semaphore()
    for d in order(outer):
        pl.semaphore_signal(
            barrier, inc=1, device_id={"seq": far_peer(d) * INNER + r}, device_id_type=MESH
        )
    for d in order(INNER):
        pl.semaphore_signal(
            barrier, inc=1, device_id={"seq": z * INNER + row_peer(d)}, device_id_type=MESH
        )

    loads = {}
    for k, (src, dst) in enumerate(((fade_h, fade_v), (upd_h, upd_v), (gate_h, gate_v))):
        for b in range(batch):
            for p in range(parts):
                at = (b, pl.ds(p * rows, rows))
                loads[k, b, p] = pltpu.make_async_copy(
                    src.at[at], dst.at[at], load_sem.at[k, b, p]
                )
    for k in range(3):
        for b in range(batch):
            for p in range(parts):
                loads[k, b, p].start()

    lower[...] = triangle(rows, False)
    upper[...] = triangle(rows, True)
    scale = 1.0 / total_length

    for b in range(batch):
        passed = jnp.zeros((1, width), jnp.float32)
        sums = jnp.zeros((1, width), jnp.float32)
        back = jnp.zeros((1, width), jnp.float32)
        for p in range(parts):
            at = (b, slice(p * rows, (p + 1) * rows))
            loads[0, b, p].wait()
            fade = fade_v[at]
            log = running(lower[...], fade) + passed
            logs[at] = log
            loads[1, b, p].wait()
            push = upd_v[at].astype(jnp.float32)
            sums = sums + jnp.sum(jnp.exp(log * scale) * push, axis=0, keepdims=True)
            back = back + jnp.sum(jnp.exp((fade - log) * scale) * push, axis=0, keepdims=True)
            passed = log[rows - 1 :, :]
        keep = jnp.exp(-passed * scale)
        for t in range(tiles):
            i, cut = b * tiles + t, slice(t * LANES, (t + 1) * LANES)
            row_out[i : i + 1, :] = keep[:, cut]
            row_out[quantity + i : quantity + i + 1, :] = (keep * sums)[:, cut]
            row_out[2 * quantity + i : 2 * quantity + i + 1, :] = back[:, cut]

    pl.semaphore_wait(barrier, outer - 1 + INNER - 1)
    row_copies = []
    for d in order(INNER):
        row_copies.append(
            pltpu.make_async_remote_copy(
                src_ref=row_out,
                dst_ref=row_in.at[r],
                send_sem=row_send.at[d],
                recv_sem=row_recv.at[r],
                device_id={"seq": z * INNER + row_peer(d)},
                device_id_type=MESH,
            )
        )
        row_copies[-1].start()

    for b in range(batch):
        passed = jnp.zeros((1, width), jnp.float32)
        for p in range(parts):
            at = (b, slice(p * rows, (p + 1) * rows))
            log = logs[at]
            push = upd_v[at].astype(jnp.float32)
            run = running(lower[...], jnp.exp(log * scale) * push) + passed
            passed = run[rows - 1 :, :]
            base[at] = run * jnp.exp(-log * scale)

    own = row_out[...]
    row_in[pl.ds(r, 1)] = own[None]
    for d in range(1, INNER):
        slot = row_peer(d)
        pltpu.make_async_remote_copy(
            src_ref=row_out,
            dst_ref=row_in.at[slot],
            send_sem=row_send.at[d],
            recv_sem=row_recv.at[slot],
            device_id={"seq": z * INNER + slot},
            device_id_type=MESH,
        ).wait_recv()

    def parts_of(share):
        return share[:quantity], share[quantity : 2 * quantity], share[2 * quantity :]

    shares = [parts_of(row_in[k]) for k in range(INNER)]
    zero, one = jnp.zeros((quantity, LANES), jnp.float32), jnp.ones((quantity, LANES), jnp.float32)
    keep_row, forward_row, backward_row = one, zero, zero
    keep_before, forward_before = one, zero
    for k in range(INNER):
        keep, forward, _ = shares[k]
        forward_row = keep * forward_row + forward
        keep_row = keep * keep_row
        keep_before = jnp.where(k < r, keep_row, keep_before)
        forward_before = jnp.where(k < r, forward_row, forward_before)
    keep_part, keep_after, backward_after = one, one, zero
    for k in reversed(range(INNER)):
        keep, _, backward = shares[k]
        backward_row = keep * backward_row + backward
        keep_part = keep * keep_part
        keep_after = jnp.where(k > r, keep_part, keep_after)
        backward_after = jnp.where(k > r, backward_row, backward_after)
    for k, last in enumerate((forward_row, backward_row)):
        far_out[k, :quantity] = keep_row
        far_out[k, quantity:] = last

    far_copies = []
    for d in order(outer):
        way = jnp.where(far_peer(d) > z, 0, 1)
        far_copies.append(
            pltpu.make_async_remote_copy(
                src_ref=far_out.at[way],
                dst_ref=far_in.at[z],
                send_sem=far_send.at[d],
                recv_sem=far_recv.at[z],
                device_id={"seq": far_peer(d) * INNER + r},
                device_id_type=MESH,
            )
        )
        far_copies[-1].start()

    own_keep = own[:quantity]
    for b in range(batch):
        passed = jnp.zeros((1, width), jnp.float32)
        for p in reversed(range(parts)):
            at = (b, slice(p * rows, (p + 1) * rows))
            log = logs[at]
            before = log - fade_v[at]
            push = upd_v[at].astype(jnp.float32)
            run = running(upper[...], jnp.exp(-before * scale) * push) + passed
            passed = run[:1, :]
            loads[2, b, p].wait()
            gate = gate_v[at].astype(jnp.float32)
            gate = gate * (total_length**-0.5) / (1.0 + jnp.exp(-gate))
            raised = jnp.exp(before * scale) * gate
            base[at] = base[at] * gate + run * raised
            qv[at] = jnp.exp(-log * scale) * gate
            rv[at] = raised

    far_in[pl.ds(z, 1)] = far_out[0:1]
    for d in range(1, outer):
        slot = far_peer(d)
        pltpu.make_async_remote_copy(
            src_ref=far_out.at[0],
            dst_ref=far_in.at[slot],
            send_sem=far_send.at[d],
            recv_sem=far_recv.at[slot],
            device_id={"seq": slot * INNER + r},
            device_id_type=MESH,
        ).wait_recv()
    enter_forward, enter_backward = zero, zero
    for k in range(outer):
        share = far_in[k]
        new = share[:quantity] * enter_forward + share[quantity:]
        enter_forward = jnp.where(k < z, new, enter_forward)
    for k in reversed(range(outer)):
        share = far_in[k]
        new = share[:quantity] * enter_backward + share[quantity:]
        enter_backward = jnp.where(k > z, new, enter_backward)
    enter_forward = keep_before * enter_forward + forward_before
    enter_backward = own_keep * (keep_after * enter_backward + backward_after)

    for b in range(batch):
        for t in range(tiles):
            i, cut = b * tiles + t, slice(t * LANES, (t + 1) * LANES)
            ahead, behind = enter_forward[i : i + 1], enter_backward[i : i + 1]
            out_ref[b, :, cut] = (
                base[b, :, cut] + qv[b, :, cut] * ahead + rv[b, :, cut] * behind
            ).astype(out_ref.dtype)

    for copy in row_copies + far_copies:
        copy.wait_send()


def local(outer, total_length, fade_rate, update_in, gate_in):
    batch, length, width = fade_rate.shape
    rows = min(256, length)
    parts = length // rows
    quantity = batch * width // LANES
    full, f32 = (batch, length, width), jnp.float32
    return pl.pallas_call(
        functools.partial(kernel, outer, total_length, rows),
        out_shape=jax.ShapeDtypeStruct(full, update_in.dtype),
        in_specs=[pl.BlockSpec(memory_space=pltpu.HBM)] * 3,
        out_specs=pl.BlockSpec(memory_space=pltpu.VMEM),
        scratch_shapes=[
            pltpu.VMEM(full, f32),
            pltpu.VMEM(full, update_in.dtype),
            pltpu.VMEM(full, gate_in.dtype),
            pltpu.VMEM((rows, rows), jnp.bfloat16),
            pltpu.VMEM((rows, rows), jnp.bfloat16),
            pltpu.VMEM(full, f32),
            pltpu.VMEM(full, f32),
            pltpu.VMEM(full, f32),
            pltpu.VMEM(full, f32),
            pltpu.VMEM((3 * quantity, LANES), f32),
            pltpu.VMEM((INNER, 3 * quantity, LANES), f32),
            pltpu.VMEM((2, 2 * quantity, LANES), f32),
            pltpu.VMEM((outer, 2 * quantity, LANES), f32),
            pltpu.SemaphoreType.DMA((3, batch, parts)),
            pltpu.SemaphoreType.DMA((INNER,)),
            pltpu.SemaphoreType.DMA((INNER,)),
            pltpu.SemaphoreType.DMA((outer,)),
            pltpu.SemaphoreType.DMA((outer,)),
        ],
        compiler_params=pltpu.CompilerParams(
            collective_id=0, has_side_effects=True, vmem_limit_bytes=32 * 2**20
        ),
    )(*(pltpu.with_memory_space_constraint(a, pltpu.HBM) for a in (fade_rate, update_in, gate_in)))


def solution(mesh):
    spec = P(None, "seq", "width")
    devices = mesh.shape["seq"]

    def step(fade_rate, update_in, gate_in):
        body = functools.partial(local, devices // INNER, fade_rate.shape[1])
        return jax.shard_map(
            body, mesh=mesh, in_specs=(spec, spec, spec), out_specs=spec, check_vma=False
        )(fade_rate, update_in, gate_in)

    return step
```

```python
import functools
import math

import jax
import jax.numpy as jnp
from jax import lax
from jax.experimental import pallas as pl
from jax.experimental.pallas import tpu as pltpu
from jax.sharding import PartitionSpec as P

MESH = pl.DeviceIdType.MESH
INNER = 8
LANES = 128
ROWS = 128
SUB = 8


def triangle(rows, upper):
    r = lax.broadcasted_iota(jnp.int32, (rows, rows), 0)
    c = lax.broadcasted_iota(jnp.int32, (rows, rows), 1)
    inside = c >= r if upper else c <= r
    return jnp.where(inside, 1.0, 0.0).astype(jnp.bfloat16)


dot = functools.partial(jnp.dot, preferred_element_type=jnp.float32)


def running(mask, value):
    high = value.astype(jnp.bfloat16)
    low = (value - high.astype(jnp.float32)).astype(jnp.bfloat16)
    return dot(mask, high) + dot(mask, low)


def folded(value):
    return jnp.sum(value.reshape(value.shape[0] // SUB, SUB, value.shape[1]), axis=0)


def kernel(
    outer, total_length,
    fade_h, upd_h, gate_h, out_ref,
    fade_v, upd_v, gate_v, lower, upper, logs, base, qv, rv, into,
    row_out, row_in, far_out, far_in,
    load_sem, row_send, row_recv, far_send, far_recv, near_sem, next_sem,
):
    batch, length, width = fade_v.shape
    parts = length // ROWS
    tiles = width // LANES
    quantity = batch * tiles
    seq = lax.axis_index("seq")
    z, r = seq // INNER, seq % INNER

    def row_peer(d):
        return {"seq": z * INNER + (r + d) % INNER}

    def far_peer(d):
        return {"seq": ((z + d) % outer) * INNER + r}

    def order(count):
        return sorted(range(1, count), key=lambda d: -min(d, count - d))

    def signal(sem, peer):
        pl.semaphore_signal(sem, inc=1, device_id=peer, device_id_type=MESH)

    half = length // 2
    arrays = ((fade_h, fade_v), (upd_h, upd_v), (gate_h, gate_v))
    for b in range(batch):
        for k in range(2):
            for h in range(2):
                at = (b, pl.ds(h * half, half))
                src, dst = arrays[k]
                pltpu.make_async_copy(src.at[at], dst.at[at], load_sem.at[k, b]).start()

    def loaded(k, b):
        src, dst = arrays[k]
        pltpu.make_async_copy(src.at[b], dst.at[b], load_sem.at[k, b]).wait()

    barrier = pltpu.get_barrier_semaphore()
    for d in order(INNER):
        signal(barrier, row_peer(d))
    for d in (1, outer - 1):
        signal(barrier, far_peer(d))
    for b in range(batch):
        src, dst = arrays[2]
        pltpu.make_async_copy(src.at[b], dst.at[b], load_sem.at[2, b]).start()

    lower[...] = triangle(ROWS, False)
    scale = math.log2(math.e) / total_length

    totals = {}
    for b in range(batch):
        loaded(0, b)
        loaded(1, b)
        ups, downs = [], []
        for p in range(parts):
            at = (b, slice(p * ROWS, (p + 1) * ROWS))
            fade = fade_v[at]
            log = dot(lower[...], fade.astype(jnp.bfloat16))
            logs[at] = log
            push = upd_v[at].astype(jnp.float32)
            ups.append(folded(jnp.exp2(log * scale) * push))
            downs.append(folded(jnp.exp2((fade - log) * scale) * push))
            total = jnp.sum(folded(fade), axis=0, keepdims=True)
            totals[b, p] = total
        keeps = [jnp.exp2(totals[b, p] * -scale) for p in range(parts)]
        state = jnp.zeros((SUB, width), jnp.float32)
        for p in range(parts):
            into[0, b, p] = state
            state = keeps[p] * (state + ups[p])
        forward = jnp.sum(state, axis=0, keepdims=True)
        state = jnp.zeros((SUB, width), jnp.float32)
        for p in reversed(range(parts)):
            into[1, b, p] = keeps[p] * state
            state = downs[p] + keeps[p] * state
        backward = jnp.sum(state, axis=0, keepdims=True)
        keep = jnp.exp2(sum(totals[b, p] for p in range(parts)) * -scale)
        for t in range(tiles):
            i, cut = b * tiles + t, slice(t * LANES, (t + 1) * LANES)
            row_out[i : i + 1, :] = keep[:, cut]
            row_out[quantity + i : quantity + i + 1, :] = forward[:, cut]
            row_out[2 * quantity + i : 2 * quantity + i + 1, :] = backward[:, cut]

    pl.semaphore_wait(barrier, INNER - 1 + 2)
    for d in order(INNER):
        pltpu.make_async_remote_copy(
            src_ref=row_out, dst_ref=row_in.at[r], send_sem=row_send, recv_sem=row_recv,
            device_id=row_peer(d), device_id_type=MESH,
        ).start()
    for d in (1, outer - 1):
        signal(near_sem, far_peer(d))

    upper[...] = triangle(ROWS, True)

    def forward_part(b):
        for p in range(parts):
            at = (b, slice(p * ROWS, (p + 1) * ROWS))
            log = logs[at] * scale
            push = upd_v[at].astype(jnp.float32)
            enter = jnp.sum(into[0, b, p], axis=0, keepdims=True)
            run = running(lower[...], jnp.exp2(log) * push) + enter
            base[at] = run * jnp.exp2(-log)

    forward_part(0)
    pl.semaphore_wait(near_sem, 2)
    for d in (2, outer - 2):
        signal(next_sem, far_peer(d))
    for b in range(1, batch):
        forward_part(b)

    own = row_out[...]
    row_in[pl.ds(r, 1)] = own[None]
    others = row_in.at[pl.ds(0, INNER - 1)]
    pltpu.make_async_copy(others, others, row_recv).wait()

    def parts_of(share):
        return share[:quantity], share[quantity : 2 * quantity], share[2 * quantity :]

    shares = [parts_of(row_in[k]) for k in range(INNER)]
    zero, one = jnp.zeros((quantity, LANES), jnp.float32), jnp.ones((quantity, LANES), jnp.float32)
    keep_row, forward_row, backward_row = one, zero, zero
    keep_before, forward_before = one, zero
    for k in range(INNER):
        keep, forward, _ = shares[k]
        forward_row = keep * forward_row + forward
        keep_row = keep * keep_row
        keep_before = jnp.where(k < r, keep_row, keep_before)
        forward_before = jnp.where(k < r, forward_row, forward_before)
    keep_part, keep_after, backward_after = one, one, zero
    for k in reversed(range(INNER)):
        keep, _, backward = shares[k]
        backward_row = keep * backward_row + backward
        keep_part = keep * keep_part
        keep_after = jnp.where(k > r, keep_part, keep_after)
        backward_after = jnp.where(k > r, backward_row, backward_after)
    for k, last in enumerate((forward_row, backward_row)):
        far_out[k, :quantity] = keep_row
        far_out[k, quantity:] = last

    pl.semaphore_wait(next_sem, 2)
    for d in order(outer):
        way = jnp.where((z + d) % outer > z, 0, 1)
        pltpu.make_async_remote_copy(
            src_ref=far_out.at[way], dst_ref=far_in.at[z], send_sem=far_send, recv_sem=far_recv,
            device_id=far_peer(d), device_id_type=MESH,
        ).start()

    for b in range(batch):
        loaded(2, b)
        before = jnp.zeros((1, width), jnp.float32)
        for p in range(parts):
            at = (b, slice(p * ROWS, (p + 1) * ROWS))
            log = logs[at] * scale
            short = log - fade_v[at] * scale
            push = upd_v[at].astype(jnp.float32)
            enter = jnp.sum(into[1, b, p], axis=0, keepdims=True)
            run = running(upper[...], jnp.exp2(-short) * push) + enter
            gate = gate_v[at].astype(jnp.float32)
            gate = gate * (total_length**-0.5) / (1.0 + jnp.exp(-gate))
            raised = jnp.exp2(short) * gate
            base[at] = base[at] * gate + run * raised
            after = sum(totals[b, q] for q in range(p, parts))
            qv[at] = jnp.exp2(-log) * gate * jnp.exp2(before * -scale)
            rv[at] = raised * jnp.exp2(after * -scale)
            before = before + totals[b, p]

    far_in[pl.ds(z, 1)] = far_out[0:1]
    others = far_in.at[pl.ds(0, outer - 1)]
    pltpu.make_async_copy(others, others, far_recv).wait()
    enter_forward, enter_backward = zero, zero
    for k in range(outer):
        share = far_in[k]
        new = share[:quantity] * enter_forward + share[quantity:]
        enter_forward = jnp.where(k < z, new, enter_forward)
    for k in reversed(range(outer)):
        share = far_in[k]
        new = share[:quantity] * enter_backward + share[quantity:]
        enter_backward = jnp.where(k > z, new, enter_backward)
    enter_forward = keep_before * enter_forward + forward_before
    enter_backward = keep_after * enter_backward + backward_after

    for b in range(batch):
        for t in range(tiles):
            i, cut = b * tiles + t, slice(t * LANES, (t + 1) * LANES)
            ahead, behind = enter_forward[i : i + 1], enter_backward[i : i + 1]
            out_ref[b, :, cut] = (
                base[b, :, cut] + qv[b, :, cut] * ahead + rv[b, :, cut] * behind
            ).astype(out_ref.dtype)

    for refs, count, sem in ((row_in, INNER, row_send), (far_in, outer, far_send)):
        sent = refs.at[pl.ds(0, count - 1)]
        pltpu.make_async_copy(sent, sent, sem).wait()


def local(outer, total_length, fade_rate, update_in, gate_in):
    batch, length, width = fade_rate.shape
    quantity = batch * width // LANES
    full, f32 = (batch, length, width), jnp.float32
    arguments = (fade_rate, update_in, gate_in)
    return pl.pallas_call(
        functools.partial(kernel, outer, total_length),
        out_shape=jax.ShapeDtypeStruct(full, update_in.dtype),
        in_specs=[pl.BlockSpec(memory_space=pltpu.HBM)] * 3,
        out_specs=pl.BlockSpec(memory_space=pltpu.VMEM),
        scratch_shapes=[
            pltpu.VMEM(full, f32),
            pltpu.VMEM(full, update_in.dtype),
            pltpu.VMEM(full, gate_in.dtype),
            pltpu.VMEM((ROWS, ROWS), jnp.bfloat16),
            pltpu.VMEM((ROWS, ROWS), jnp.bfloat16),
            pltpu.VMEM(full, f32),
            pltpu.VMEM(full, f32),
            pltpu.VMEM(full, f32),
            pltpu.VMEM(full, f32),
            pltpu.VMEM((2, batch, length // ROWS, SUB, width), f32),
            pltpu.VMEM((3 * quantity, LANES), f32),
            pltpu.VMEM((INNER, 3 * quantity, LANES), f32),
            pltpu.VMEM((2, 2 * quantity, LANES), f32),
            pltpu.VMEM((outer, 2 * quantity, LANES), f32),
            pltpu.SemaphoreType.DMA((3, batch)),
            pltpu.SemaphoreType.DMA,
            pltpu.SemaphoreType.DMA,
            pltpu.SemaphoreType.DMA,
            pltpu.SemaphoreType.DMA,
            pltpu.SemaphoreType.REGULAR,
            pltpu.SemaphoreType.REGULAR,
        ],
        compiler_params=pltpu.CompilerParams(
            collective_id=0, has_side_effects=True, vmem_limit_bytes=32 * 2**20
        ),
    )(*(pltpu.with_memory_space_constraint(a, pltpu.HBM) for a in arguments))


def solution(mesh):
    spec = P(None, "seq", "width")
    devices = mesh.shape["seq"]

    def step(fade_rate, update_in, gate_in):
        body = functools.partial(local, devices // INNER, fade_rate.shape[1])
        return jax.shard_map(
            body, mesh=mesh, in_specs=(spec, spec, spec), out_specs=spec, check_vma=False
        )(fade_rate, update_in, gate_in)

    return step
```

```python
import functools
import math

import jax
import jax.numpy as jnp
from jax import lax
from jax.experimental import pallas as pl
from jax.experimental.pallas import tpu as pltpu
from jax.sharding import PartitionSpec as P

MESH = pl.DeviceIdType.MESH
INNER = 8
CORES = 2
CHIPS = INNER // CORES
LANES = 128
ROWS = 128
SUB = 8


def triangle(rows, upper):
    r = lax.broadcasted_iota(jnp.int32, (rows, rows), 0)
    c = lax.broadcasted_iota(jnp.int32, (rows, rows), 1)
    inside = c >= r if upper else c <= r
    return jnp.where(inside, 1.0, 0.0).astype(jnp.bfloat16)


dot = functools.partial(jnp.dot, preferred_element_type=jnp.float32)


def running(mask, value):
    high = value.astype(jnp.bfloat16)
    low = (value - high.astype(jnp.float32)).astype(jnp.bfloat16)
    return dot(mask, high) + dot(mask, low)


def folded(value):
    return jnp.sum(value.reshape(value.shape[0] // SUB, SUB, value.shape[1]), axis=0)


def kernel(
    outer, total_length,
    fade_h, upd_h, gate_h, out_ref,
    fade_v, upd_v, gate_v, lower, upper, logs, base, qv, rv, into,
    row_out, row_in, far_out, far_in,
    load_sem, gate_sem, row_send, row_recv, far_send, far_recv, told,
):
    batch, length, width = upd_v.shape
    parts = length // ROWS
    tiles = width // LANES
    seq = lax.axis_index("seq")
    z, r = seq // INNER, seq % INNER
    x, core = r // CORES, r % CORES

    def at(row, place):
        return {"seq": row * INNER + place}

    def others(own, count):
        return [k + jnp.where(k >= own, 1, 0) for k in range(count - 1)]

    def signal(sem, peer):
        pl.semaphore_signal(sem, inc=1, device_id=peer, device_id_type=MESH)

    def send(src, dst, out_sem, in_sem, peer):
        pltpu.make_async_remote_copy(
            src_ref=src, dst_ref=dst, send_sem=out_sem, recv_sem=in_sem,
            device_id=peer, device_id_type=MESH,
        ).start()

    def wait(ref, sem):
        pltpu.make_async_copy(ref, ref, sem).wait()

    def load(b):
        half = length // 2
        for h in range(2):
            part = pl.ds(h * half, half)
            to = fade_v.at[pl.ds(b * length + h * half, half)]
            pltpu.make_async_copy(fade_h.at[b, part], to, load_sem.at[b]).start()
            to = upd_v.at[b, part]
            pltpu.make_async_copy(upd_h.at[b, part], to, load_sem.at[b]).start()

    def loaded(b):
        wait(fade_v.at[pl.ds(0, length + length // 2)], load_sem.at[b])

    load(0)
    barrier = pltpu.get_barrier_semaphore()
    for d in range(1, CHIPS):
        signal(barrier, at(z, (x + d) % CHIPS * CORES + 1))

    @pl.when(core == 0)
    def _():
        signal(barrier, at(z, r + 1))

    load(1)
    for row in others(z, outer):
        signal(barrier, at(row, x * CORES))
    lower[...] = triangle(ROWS, False)
    scale = math.log2(math.e) / total_length
    partner = at(z, r + 1 - 2 * core)

    totals = {}

    def summary(b):
        ups, downs = [], []
        for p in range(parts):
            cut = (b, slice(p * ROWS, (p + 1) * ROWS))
            fade = fade_v[b * length + p * ROWS : b * length + (p + 1) * ROWS] * scale
            log = dot(lower[...], fade.astype(jnp.bfloat16))
            logs[cut] = log
            push = upd_v[cut].astype(jnp.float32)
            ups.append(folded(jnp.exp2(log) * push))
            downs.append(folded(jnp.exp2(fade - log) * push))
            totals[b, p] = jnp.sum(folded(fade), axis=0, keepdims=True)
        keeps = [jnp.exp2(-totals[b, p]) for p in range(parts)]
        state = jnp.zeros((SUB, width), jnp.float32)
        for p in range(parts):
            into[0, b, p] = state
            state = keeps[p] * (state + ups[p])
        forward = jnp.sum(state, axis=0, keepdims=True)
        state = jnp.zeros((SUB, width), jnp.float32)
        for p in reversed(range(parts)):
            into[1, b, p] = keeps[p] * state
            state = downs[p] + keeps[p] * state
        backward = jnp.sum(state, axis=0, keepdims=True)
        keep = jnp.exp2(-sum(totals[b, p] for p in range(parts)))
        for k, value in enumerate((keep, forward, backward)):
            for t in range(tiles):
                i = k * tiles + t
                row_out[b, i : i + 1, :] = value[:, t * LANES : (t + 1) * LANES]

    def send_row(b):
        own = (1 - core) * CHIPS + x
        for k in others(own, INNER):
            place = k % CHIPS * CORES + 1 - k // CHIPS
            send(row_out.at[b], row_in.at[b, r], row_send.at[b], row_recv.at[b], at(z, place))

    loaded(0)
    summary(0)

    @pl.when(core == 1)
    def _():
        pl.semaphore_wait(barrier, INNER - 1)
        signal(told, partner)

    @pl.when(core == 0)
    def _():
        pl.semaphore_wait(told, 1)

    send_row(0)
    for b in range(1, batch):
        loaded(b)
        if b == batch - 1:
            pltpu.make_async_copy(gate_h, gate_v, gate_sem).start()
        summary(b)
        send_row(b)

    upper[...] = triangle(ROWS, True)

    for b in range(batch):
        for p in range(parts):
            cut = (b, slice(p * ROWS, (p + 1) * ROWS))
            log = logs[cut]
            push = upd_v[cut].astype(jnp.float32)
            enter = jnp.sum(into[0, b, p], axis=0, keepdims=True)
            run = running(lower[...], jnp.exp2(log) * push) + enter
            base[cut] = run * jnp.exp2(-log)

    @pl.when(core == 0)
    def _():
        pl.semaphore_wait(barrier, CORES * (outer - 1))
        signal(told, partner)

    @pl.when(core == 1)
    def _():
        pl.semaphore_wait(told, 1)

    zero, one = jnp.zeros((tiles, LANES), jnp.float32), jnp.ones((tiles, LANES), jnp.float32)

    def combine_row(b):
        row_in[b, pl.ds(r, 1)] = row_out[b][None]
        wait(row_in.at[b, pl.ds(0, INNER - 1)], row_recv.at[b])
        shares = [row_in[b, k] for k in range(INNER)]
        shares = [(s[:tiles], s[tiles : 2 * tiles], s[2 * tiles :]) for s in shares]
        keep_row, forward_row, backward_row = one, zero, zero
        keep_before, forward_before = one, zero
        for k in range(INNER):
            keep, forward, _ = shares[k]
            forward_row = keep * forward_row + forward
            keep_row = keep * keep_row
            keep_before = jnp.where(k < r, keep_row, keep_before)
            forward_before = jnp.where(k < r, forward_row, forward_before)
        keep_part, keep_after, backward_after = one, one, zero
        for k in reversed(range(INNER)):
            keep, _, backward = shares[k]
            backward_row = keep * backward_row + backward
            keep_part = keep * keep_part
            keep_after = jnp.where(k > r, keep_part, keep_after)
            backward_after = jnp.where(k > r, backward_row, backward_after)
        for k, last in enumerate((forward_row, backward_row)):
            far_out[b, k, :tiles] = keep_row
            far_out[b, k, tiles:] = last

        @pl.when(core == 1)
        def _():
            for row in others(z, outer):
                way = jnp.where(row > z, 0, 1)
                for c in (1, 0):
                    send(
                        far_out.at[b, way], far_in.at[b, z], far_send, far_recv.at[b],
                        at(row, x * CORES + c),
                    )

        return keep_before, forward_before, keep_after, backward_after

    inside = [combine_row(b) for b in range(batch)]

    wait(gate_v, gate_sem)
    for b in range(batch):
        before = jnp.zeros((1, width), jnp.float32)
        for p in range(parts):
            cut = (b, slice(p * ROWS, (p + 1) * ROWS))
            log = logs[cut]
            short = log - fade_v[b * length + p * ROWS : b * length + (p + 1) * ROWS] * scale
            push = upd_v[cut].astype(jnp.float32)
            enter = jnp.sum(into[1, b, p], axis=0, keepdims=True)
            run = running(upper[...], jnp.exp2(-short) * push) + enter
            gate = gate_v[cut].astype(jnp.float32)
            gate = gate * (total_length**-0.5) / (1.0 + jnp.exp(-gate))
            raised = jnp.exp2(short) * gate
            base[cut] = base[cut] * gate + run * raised
            after = sum(totals[b, q] for q in range(p, parts))
            qv[cut] = jnp.exp2(-log) * gate * jnp.exp2(-before)
            rv[cut] = raised * jnp.exp2(-after)
            before = before + totals[b, p]

    for b in range(batch):
        far_in[b, pl.ds(z, 1)] = far_out[b, 0:1]
        wait(far_in.at[b, pl.ds(0, outer - 1)], far_recv.at[b])
        keep_before, forward_before, keep_after, backward_after = inside[b]
        shares = [far_in[b, k] for k in range(outer)]
        enter_forward, enter_backward = zero, zero
        for k in range(outer):
            new = shares[k][:tiles] * enter_forward + shares[k][tiles:]
            enter_forward = jnp.where(k < z, new, enter_forward)
        for k in reversed(range(outer)):
            new = shares[k][:tiles] * enter_backward + shares[k][tiles:]
            enter_backward = jnp.where(k > z, new, enter_backward)
        enter_forward = keep_before * enter_forward + forward_before
        enter_backward = keep_after * enter_backward + backward_after
        for t in range(tiles):
            cut = slice(t * LANES, (t + 1) * LANES)
            ahead, behind = enter_forward[t : t + 1], enter_backward[t : t + 1]
            out_ref[b, :, cut] = (
                base[b, :, cut] + qv[b, :, cut] * ahead + rv[b, :, cut] * behind
            ).astype(out_ref.dtype)

    for b in range(batch):
        wait(row_in.at[b, pl.ds(0, INNER - 1)], row_send.at[b])

    @pl.when(core == 1)
    def _():
        sent = batch * CORES * (outer - 1) * 2 * tiles * LANES // width
        wait(fade_v.at[pl.ds(0, sent)], far_send)


def local(outer, total_length, fade_rate, update_in, gate_in):
    batch, length, width = fade_rate.shape
    tiles = width // LANES
    full, f32 = (batch, length, width), jnp.float32
    arguments = (fade_rate, update_in, gate_in)
    return pl.pallas_call(
        functools.partial(kernel, outer, total_length),
        out_shape=jax.ShapeDtypeStruct(full, update_in.dtype),
        in_specs=[pl.BlockSpec(memory_space=pltpu.HBM)] * 3,
        out_specs=pl.BlockSpec(memory_space=pltpu.VMEM),
        scratch_shapes=[
            pltpu.VMEM((batch * length, width), f32),
            pltpu.VMEM(full, update_in.dtype),
            pltpu.VMEM(full, gate_in.dtype),
            pltpu.VMEM((ROWS, ROWS), jnp.bfloat16),
            pltpu.VMEM((ROWS, ROWS), jnp.bfloat16),
            pltpu.VMEM(full, f32),
            pltpu.VMEM(full, f32),
            pltpu.VMEM(full, f32),
            pltpu.VMEM(full, f32),
            pltpu.VMEM((2, batch, length // ROWS, SUB, width), f32),
            pltpu.VMEM((batch, 3 * tiles, LANES), f32),
            pltpu.VMEM((batch, INNER, 3 * tiles, LANES), f32),
            pltpu.VMEM((batch, 2, 2 * tiles, LANES), f32),
            pltpu.VMEM((batch, outer, 2 * tiles, LANES), f32),
            pltpu.SemaphoreType.DMA((batch,)),
            pltpu.SemaphoreType.DMA,
            pltpu.SemaphoreType.DMA((batch,)),
            pltpu.SemaphoreType.DMA((batch,)),
            pltpu.SemaphoreType.DMA,
            pltpu.SemaphoreType.DMA((batch,)),
            pltpu.SemaphoreType.REGULAR,
        ],
        compiler_params=pltpu.CompilerParams(
            collective_id=0, has_side_effects=True, vmem_limit_bytes=32 * 2**20
        ),
    )(*(pltpu.with_memory_space_constraint(a, pltpu.HBM) for a in arguments))


def solution(mesh):
    spec = P(None, "seq", "width")
    devices = mesh.shape["seq"]

    def step(fade_rate, update_in, gate_in):
        body = functools.partial(local, devices // INNER, fade_rate.shape[1])
        return jax.shard_map(
            body, mesh=mesh, in_specs=(spec, spec, spec), out_specs=spec, check_vma=False
        )(fade_rate, update_in, gate_in)

    return step
```

```python
import functools
import math

import jax
import jax.numpy as jnp
from jax import lax
from jax.experimental import pallas as pl
from jax.experimental.pallas import tpu as pltpu
from jax.sharding import PartitionSpec as P

MESH = pl.DeviceIdType.MESH
INNER = 8
CORES = 2
CHIPS = INNER // CORES
LANES = 128
ROWS = 128
SUB = 8


def triangle(rows, upper):
    r = lax.broadcasted_iota(jnp.int32, (rows, rows), 0)
    c = lax.broadcasted_iota(jnp.int32, (rows, rows), 1)
    inside = c >= r if upper else c <= r
    return jnp.where(inside, 1.0, 0.0).astype(jnp.bfloat16)


dot = functools.partial(jnp.dot, preferred_element_type=jnp.float32)


def running(mask, value):
    high = value.astype(jnp.bfloat16)
    low = (value - high.astype(jnp.float32)).astype(jnp.bfloat16)
    return dot(mask, high) + dot(mask, low)


def folded(value):
    return jnp.sum(value.reshape(value.shape[0] // SUB, SUB, value.shape[1]), axis=0)


def kernel(
    outer, total_length,
    fade_h, upd_h, gate_h, out_ref,
    fade_v, upd_v, gate_v, lower, upper, logs, base, qv, rv, into,
    row_out, row_in, last_out, last_in, far_out, far_in,
    load_sem, gate_sem, row_send, row_recv, last_send, last_recv, far_send, far_recv, told,
):
    batch, length, width = upd_v.shape
    parts = length // ROWS
    tiles = width // LANES
    seq = lax.axis_index("seq")
    z, r = seq // INNER, seq % INNER
    x, core = r // CORES, r % CORES

    def at(row, place):
        return {"seq": row * INNER + place}

    def others(own, count):
        return [k + jnp.where(k >= own, 1, 0) for k in range(count - 1)]

    def signal(sem, peer):
        pl.semaphore_signal(sem, inc=1, device_id=peer, device_id_type=MESH)

    def send(src, dst, out_sem, in_sem, peer):
        pltpu.make_async_remote_copy(
            src_ref=src, dst_ref=dst, send_sem=out_sem, recv_sem=in_sem,
            device_id=peer, device_id_type=MESH,
        ).start()

    def wait(ref, sem):
        pltpu.make_async_copy(ref, ref, sem).wait()

    def load(b):
        half = length // 2
        for h in range(2):
            part = pl.ds(h * half, half)
            to = fade_v.at[pl.ds(b * length + h * half, half)]
            pltpu.make_async_copy(fade_h.at[b, part], to, load_sem.at[b]).start()
            to = upd_v.at[b, part]
            pltpu.make_async_copy(upd_h.at[b, part], to, load_sem.at[b]).start()

    def loaded(b):
        wait(fade_v.at[pl.ds(0, length + length // 2)], load_sem.at[b])

    load(0)
    barrier = pltpu.get_barrier_semaphore()
    for d in range(1, CHIPS):
        signal(barrier, at(z, (x + d) % CHIPS * CORES + 1))

    @pl.when(core == 0)
    def _():
        signal(barrier, at(z, r + 1))

    load(1)
    for row in others(z, outer):
        signal(barrier, at(row, x * CORES))
    lower[...] = triangle(ROWS, False)
    scale = math.log2(math.e) / total_length
    partner = at(z, r + 1 - 2 * core)

    totals, entering = {}, {}

    def summary(b):
        downs = []
        for p in range(parts):
            cut = (b, slice(p * ROWS, (p + 1) * ROWS))
            fade = fade_v[b * length + p * ROWS : b * length + (p + 1) * ROWS] * scale
            log = dot(lower[...], fade.astype(jnp.bfloat16))
            logs[cut] = log
            downs.append(folded(jnp.exp2(fade - log) * upd_v[cut].astype(jnp.float32)))
            totals[b, p] = jnp.sum(folded(fade), axis=0, keepdims=True)
        state = jnp.zeros((SUB, width), jnp.float32)
        for p in reversed(range(parts)):
            entering[b, p] = jnp.exp2(-totals[b, p]) * state
            state = downs[p] + entering[b, p]
            into[b, p] = entering[b, p]
        backward = jnp.sum(state, axis=0, keepdims=True)
        keep = jnp.exp2(-sum(totals[b, p] for p in range(parts)))
        for k, value in enumerate((keep, backward)):
            for t in range(tiles):
                i = k * tiles + t
                row_out[b, i : i + 1, :] = value[:, t * LANES : (t + 1) * LANES]

    def send_row(src, dst, out_sem, in_sem):
        own = (1 - core) * CHIPS + x
        for k in others(own, INNER):
            place = k % CHIPS * CORES + 1 - k // CHIPS
            send(src, dst.at[r], out_sem, in_sem, at(z, place))

    def send_backward(b):
        send_row(row_out.at[b], row_in.at[b], row_send.at[b], row_recv.at[b])

    loaded(0)
    summary(0)

    @pl.when(core == 1)
    def _():
        pl.semaphore_wait(barrier, INNER - 1)
        signal(told, partner)

    @pl.when(core == 0)
    def _():
        pl.semaphore_wait(told, 1)

    send_backward(0)
    for b in range(1, batch):
        loaded(b)
        if b == batch - 1:
            pltpu.make_async_copy(gate_h, gate_v, gate_sem).start()
        summary(b)
        send_backward(b)

    upper[...] = triangle(ROWS, True)

    for b in range(batch):
        state = jnp.zeros((1, width), jnp.float32)
        for p in range(parts):
            cut = (b, slice(p * ROWS, (p + 1) * ROWS))
            log = logs[cut]
            push = upd_v[cut].astype(jnp.float32)
            run = running(lower[...], jnp.exp2(log) * push) + state
            state = run[ROWS - 1 :] * jnp.exp2(-totals[b, p])
            base[cut] = run * jnp.exp2(-log)
        for t in range(tiles):
            i = b * tiles + t
            last_out[i : i + 1, :] = state[:, t * LANES : (t + 1) * LANES]
    send_row(last_out, last_in, last_send, last_recv)

    @pl.when(core == 0)
    def _():
        pl.semaphore_wait(barrier, CORES * (outer - 1))
        signal(told, partner)

    @pl.when(core == 1)
    def _():
        pl.semaphore_wait(told, 1)

    zero, one = jnp.zeros((tiles, LANES), jnp.float32), jnp.ones((tiles, LANES), jnp.float32)

    def send_far(b, way, row):
        for c in (1, 0):
            send(
                far_out.at[b, way], far_in.at[b, z], far_send, far_recv.at[b],
                at(row, x * CORES + c),
            )

    before, after = {}, {}
    for b in range(batch):
        row_in[b, pl.ds(r, 1)] = row_out[b][None]
        wait(row_in.at[b, pl.ds(0, INNER - 1)], row_recv.at[b])
        shares = [row_in[b, k] for k in range(INNER)]
        keep_row, backward_row, keep_after, backward_after = one, zero, one, zero
        for k in reversed(range(INNER)):
            backward_row = shares[k][:tiles] * backward_row + shares[k][tiles:]
            keep_row = shares[k][:tiles] * keep_row
            keep_after = jnp.where(k > r, keep_row, keep_after)
            backward_after = jnp.where(k > r, backward_row, backward_after)
        after[b] = keep_after, backward_after
        far_out[b, 0, :tiles] = keep_row
        far_out[b, 1, :tiles] = keep_row
        far_out[b, 1, tiles:] = backward_row
        for row in range(outer - 1):

            @pl.when((core == 1) & (row < z))
            def _():
                send_far(b, 1, row)

    last_in[pl.ds(r, 1)] = last_out[...][None]
    wait(last_in.at[pl.ds(0, INNER - 1)], last_recv)
    for b in range(batch):
        keep_row, forward_row, keep_before, forward_before = one, zero, one, zero
        for k in range(INNER):
            keep = row_in[b, k, :tiles]
            forward_row = keep * forward_row + last_in[k, b * tiles : (b + 1) * tiles]
            keep_row = keep * keep_row
            keep_before = jnp.where(k < r, keep_row, keep_before)
            forward_before = jnp.where(k < r, forward_row, forward_before)
        before[b] = keep_before, forward_before
        far_out[b, 0, tiles:] = forward_row
        for row in range(1, outer):

            @pl.when((core == 1) & (row > z))
            def _():
                send_far(b, 0, row)

    wait(gate_v, gate_sem)
    for b in range(batch):
        passed = jnp.zeros((1, width), jnp.float32)
        for p in range(parts):
            cut = (b, slice(p * ROWS, (p + 1) * ROWS))
            log = logs[cut]
            short = log - fade_v[b * length + p * ROWS : b * length + (p + 1) * ROWS] * scale
            push = upd_v[cut].astype(jnp.float32)
            enter = jnp.sum(into[b, p], axis=0, keepdims=True)
            run = running(upper[...], jnp.exp2(-short) * push) + enter
            gate = gate_v[cut].astype(jnp.float32)
            gate = gate * (total_length**-0.5) / (1.0 + jnp.exp(-gate))
            raised = jnp.exp2(short) * gate
            base[cut] = base[cut] * gate + run * raised
            left = sum(totals[b, q] for q in range(p, parts))
            qv[cut] = jnp.exp2(-log) * gate * jnp.exp2(-passed)
            rv[cut] = raised * jnp.exp2(-left)
            passed = passed + totals[b, p]

    for b in range(batch):
        far_in[b, pl.ds(z, 1)] = far_out[b, 0:1]
        wait(far_in.at[b, pl.ds(0, outer - 1)], far_recv.at[b])
        keep_before, forward_before = before[b]
        keep_after, backward_after = after[b]
        shares = [far_in[b, k] for k in range(outer)]
        enter_forward, enter_backward = zero, zero
        for k in range(outer):
            new = shares[k][:tiles] * enter_forward + shares[k][tiles:]
            enter_forward = jnp.where(k < z, new, enter_forward)
        for k in reversed(range(outer)):
            new = shares[k][:tiles] * enter_backward + shares[k][tiles:]
            enter_backward = jnp.where(k > z, new, enter_backward)
        enter_forward = keep_before * enter_forward + forward_before
        enter_backward = keep_after * enter_backward + backward_after
        for t in range(tiles):
            cut = slice(t * LANES, (t + 1) * LANES)
            ahead, behind = enter_forward[t : t + 1], enter_backward[t : t + 1]
            out_ref[b, :, cut] = (
                base[b, :, cut] + qv[b, :, cut] * ahead + rv[b, :, cut] * behind
            ).astype(out_ref.dtype)

    for b in range(batch):
        wait(row_in.at[b, pl.ds(0, INNER - 1)], row_send.at[b])
    wait(last_in.at[pl.ds(0, INNER - 1)], last_send)

    @pl.when(core == 1)
    def _():
        sent = batch * CORES * (outer - 1) * 2 * tiles * LANES // width
        wait(fade_v.at[pl.ds(0, sent)], far_send)


def local(outer, total_length, fade_rate, update_in, gate_in):
    batch, length, width = fade_rate.shape
    tiles = width // LANES
    full, f32 = (batch, length, width), jnp.float32
    arguments = (fade_rate, update_in, gate_in)
    return pl.pallas_call(
        functools.partial(kernel, outer, total_length),
        out_shape=jax.ShapeDtypeStruct(full, update_in.dtype),
        in_specs=[pl.BlockSpec(memory_space=pltpu.HBM)] * 3,
        out_specs=pl.BlockSpec(memory_space=pltpu.VMEM),
        scratch_shapes=[
            pltpu.VMEM((batch * length, width), f32),
            pltpu.VMEM(full, update_in.dtype),
            pltpu.VMEM(full, gate_in.dtype),
            pltpu.VMEM((ROWS, ROWS), jnp.bfloat16),
            pltpu.VMEM((ROWS, ROWS), jnp.bfloat16),
            pltpu.VMEM(full, f32),
            pltpu.VMEM(full, f32),
            pltpu.VMEM(full, f32),
            pltpu.VMEM(full, f32),
            pltpu.VMEM((batch, length // ROWS, SUB, width), f32),
            pltpu.VMEM((batch, 2 * tiles, LANES), f32),
            pltpu.VMEM((batch, INNER, 2 * tiles, LANES), f32),
            pltpu.VMEM((batch * tiles, LANES), f32),
            pltpu.VMEM((INNER, batch * tiles, LANES), f32),
            pltpu.VMEM((batch, 2, 2 * tiles, LANES), f32),
            pltpu.VMEM((batch, outer, 2 * tiles, LANES), f32),
            pltpu.SemaphoreType.DMA((batch,)),
            pltpu.SemaphoreType.DMA,
            pltpu.SemaphoreType.DMA((batch,)),
            pltpu.SemaphoreType.DMA((batch,)),
            pltpu.SemaphoreType.DMA,
            pltpu.SemaphoreType.DMA,
            pltpu.SemaphoreType.DMA,
            pltpu.SemaphoreType.DMA((batch,)),
            pltpu.SemaphoreType.REGULAR,
        ],
        compiler_params=pltpu.CompilerParams(
            collective_id=0, has_side_effects=True, vmem_limit_bytes=32 * 2**20
        ),
    )(*(pltpu.with_memory_space_constraint(a, pltpu.HBM) for a in arguments))


def solution(mesh):
    spec = P(None, "seq", "width")
    devices = mesh.shape["seq"]

    def step(fade_rate, update_in, gate_in):
        body = functools.partial(local, devices // INNER, fade_rate.shape[1])
        return jax.shard_map(
            body, mesh=mesh, in_specs=(spec, spec, spec), out_specs=spec, check_vma=False
        )(fade_rate, update_in, gate_in)

    return step
```

```python
import functools
import math

import jax
import jax.numpy as jnp
from jax import lax
from jax.experimental import pallas as pl
from jax.experimental.pallas import tpu as pltpu
from jax.sharding import PartitionSpec as P

MESH = pl.DeviceIdType.MESH
INNER = 8
CORES = 2
CHIPS = INNER // CORES
LANES = 128
ROWS = 128
SUB = 8
CUTS = 4


def triangle(rows, upper):
    r = lax.broadcasted_iota(jnp.int32, (rows, rows), 0)
    c = lax.broadcasted_iota(jnp.int32, (rows, rows), 1)
    inside = c >= r if upper else c <= r
    return jnp.where(inside, 1.0, 0.0).astype(jnp.bfloat16)


dot = functools.partial(jnp.dot, preferred_element_type=jnp.float32)


def running(mask, value):
    high = value.astype(jnp.bfloat16)
    low = (value - high.astype(jnp.float32)).astype(jnp.bfloat16)
    return dot(mask, high) + dot(mask, low)


def folded(value):
    return jnp.sum(value.reshape(value.shape[0] // SUB, SUB, value.shape[1]), axis=0)


def kernel(
    outer, total_length,
    fade_h, upd_h, gate_h, base, qv, rv, carried,
    fade_v, upd_v, gate_v, lower, upper, logs, into,
    row_out, row_in, last_out, last_in, far_out, far_in, as_sent,
    load_sem, row_recv, last_recv, far_recv, sent, far_sent, told,
):
    batch, length, width = upd_v.shape
    parts = length // ROWS
    tiles = width // LANES
    seq = lax.axis_index("seq")
    z, r = seq // INNER, seq % INNER
    x, core = r // CORES, r % CORES

    def at(row, place):
        return {"seq": row * INNER + place}

    def others(own, count):
        return [k + jnp.where(k >= own, 1, 0) for k in range(count - 1)]

    def signal(sem, peer):
        pl.semaphore_signal(sem, inc=1, device_id=peer, device_id_type=MESH)

    def send(src, dst, out_sem, in_sem, peer):
        pltpu.make_async_remote_copy(
            src_ref=src, dst_ref=dst, send_sem=out_sem, recv_sem=in_sem,
            device_id=peer, device_id_type=MESH,
        ).start()

    def wait(ref, sem):
        pltpu.make_async_copy(ref, ref, sem).wait()

    def load(b):
        half = length // 2
        for h in range(2):
            part = pl.ds(h * half, half)
            to = fade_v.at[pl.ds(b * length + h * half, half)]
            pltpu.make_async_copy(fade_h.at[b, part], to, load_sem.at[b]).start()
            to = upd_v.at[b, part]
            pltpu.make_async_copy(upd_h.at[b, part], to, load_sem.at[b]).start()

    def loaded(b):
        wait(fade_v.at[pl.ds(0, length + length // 2)], load_sem.at[b])

    load(0)
    barrier = pltpu.get_barrier_semaphore()
    for d in range(1, CHIPS):
        signal(barrier, at(z, (x + d) % CHIPS * CORES + 1))

    @pl.when(core == 0)
    def _():
        signal(barrier, at(z, r + 1))

    load(1)
    for row in others(z, outer):
        signal(barrier, at(row, x * CORES))
    lower[...] = triangle(ROWS, False)
    scale = math.log2(math.e) / total_length
    partner = at(z, r + 1 - 2 * core)

    totals, entering = {}, {}

    def summary(b):
        downs = []
        for p in range(parts):
            cut = (b, slice(p * ROWS, (p + 1) * ROWS))
            fade = fade_v[b * length + p * ROWS : b * length + (p + 1) * ROWS]
            log = dot(lower[...], fade.astype(jnp.bfloat16))
            logs[cut] = log
            downs.append(folded(jnp.exp2((fade - log) * scale) * upd_v[cut].astype(jnp.float32)))
            totals[b, p] = jnp.sum(folded(fade), axis=0, keepdims=True) * scale
        state = jnp.zeros((SUB, width), jnp.float32)
        for p in reversed(range(parts)):
            entering[b, p] = jnp.exp2(-totals[b, p]) * state
            state = downs[p] + entering[b, p]
            into[b, p] = entering[b, p]
        backward = jnp.sum(state, axis=0, keepdims=True)
        keep = jnp.exp2(-sum(totals[b, p] for p in range(parts)))
        for k, value in enumerate((keep, backward)):
            for t in range(tiles):
                i = k * tiles + t
                row_out[b, i : i + 1, :] = value[:, t * LANES : (t + 1) * LANES]

    def send_row(src, dst, out_sem, in_sem):
        own = (1 - core) * CHIPS + x
        for k in others(own, INNER):
            place = k % CHIPS * CORES + 1 - k // CHIPS
            send(src, dst.at[r], out_sem, in_sem, at(z, place))

    def send_backward(b):
        send_row(row_out.at[b], row_in.at[b], sent, row_recv.at[b])

    loaded(0)
    summary(0)

    @pl.when(core == 1)
    def _():
        pl.semaphore_wait(barrier, INNER - 1)
        signal(told, partner)

    @pl.when(core == 0)
    def _():
        pl.semaphore_wait(told, 1)

    send_backward(0)
    for b in range(1, batch):
        loaded(b)
        summary(b)
        send_backward(b)

    load_gate = pltpu.make_async_copy(gate_h, gate_v, load_sem.at[0])
    load_gate.start()
    upper[...] = triangle(ROWS, True)

    for b in range(batch):
        state = jnp.zeros((1, width), jnp.float32)
        for p in range(parts):
            cut = (b, slice(p * ROWS, (p + 1) * ROWS))
            log = logs[cut] * scale
            push = upd_v[cut].astype(jnp.float32)
            run = running(lower[...], jnp.exp2(log) * push) + state
            state = run[ROWS - 1 :] * jnp.exp2(-totals[b, p])
            base[cut] = run * jnp.exp2(-log)
        for t in range(tiles):
            i = b * tiles + t
            last_out[i : i + 1, :] = state[:, t * LANES : (t + 1) * LANES]
    send_row(last_out, last_in, sent, last_recv)

    @pl.when(core == 0)
    def _():
        pl.semaphore_wait(barrier, CORES * (outer - 1))
        signal(told, partner)

    @pl.when(core == 1)
    def _():
        pl.semaphore_wait(told, 1)

    zero, one = jnp.zeros((tiles, LANES), jnp.float32), jnp.ones((tiles, LANES), jnp.float32)

    def send_far(b, way, row):
        for c in (1, 0):
            send(
                far_out.at[b, way], far_in.at[b, z], far_sent, far_recv.at[b],
                at(row, x * CORES + c),
            )

    before, after = {}, {}
    for b in range(batch):
        row_in[b, pl.ds(r, 1)] = row_out[b][None]
        wait(row_in.at[b, pl.ds(0, INNER - 1)], row_recv.at[b])
        shares = [row_in[b, k] for k in range(INNER)]
        keep_row, backward_row, keep_after, backward_after = one, zero, one, zero
        for k in reversed(range(INNER)):
            backward_row = shares[k][:tiles] * backward_row + shares[k][tiles:]
            keep_row = shares[k][:tiles] * keep_row
            keep_after = jnp.where(k > r, keep_row, keep_after)
            backward_after = jnp.where(k > r, backward_row, backward_after)
        after[b] = keep_after, backward_after
        far_out[b, 0, :tiles] = keep_row
        far_out[b, 1, :tiles] = keep_row
        far_out[b, 1, tiles:] = backward_row
        for row in range(outer - 1):

            @pl.when((core == 1) & (row < z))
            def _():
                send_far(b, 1, row)

    last_in[pl.ds(r, 1)] = last_out[...][None]
    wait(last_in.at[pl.ds(0, INNER - 1)], last_recv)
    for b in range(batch):
        keep_row, forward_row, keep_before, forward_before = one, zero, one, zero
        for k in range(INNER):
            keep = row_in[b, k, :tiles]
            forward_row = keep * forward_row + last_in[k, b * tiles : (b + 1) * tiles]
            keep_row = keep * keep_row
            keep_before = jnp.where(k < r, keep_row, keep_before)
            forward_before = jnp.where(k < r, forward_row, forward_before)
        before[b] = keep_before, forward_before
        far_out[b, 0, tiles:] = forward_row
        for row in range(1, outer):

            @pl.when((core == 1) & (row > z))
            def _():
                send_far(b, 0, row)

    load_gate.wait()
    for b in range(batch):
        passed = jnp.zeros((1, width), jnp.float32)
        for p in range(parts):
            cut = (b, slice(p * ROWS, (p + 1) * ROWS))
            log = logs[cut] * scale
            short = log - fade_v[b * length + p * ROWS : b * length + (p + 1) * ROWS] * scale
            push = upd_v[cut].astype(jnp.float32)
            enter = jnp.sum(into[b, p], axis=0, keepdims=True)
            run = running(upper[...], jnp.exp2(-short) * push) + enter
            gate = gate_v[cut].astype(jnp.float32)
            gate = gate * (total_length**-0.5) / (1.0 + jnp.exp(-gate))
            raised = jnp.exp2(short) * gate
            base[cut] = base[cut] * gate + run * raised
            left = sum(totals[b, q] for q in range(p, parts))
            qv[cut] = jnp.exp2(-log) * gate * jnp.exp2(-passed)
            rv[cut] = raised * jnp.exp2(-left)
            passed = passed + totals[b, p]

    for b in range(batch):
        far_in[b, pl.ds(z, 1)] = far_out[b, 0:1]
        wait(far_in.at[b, pl.ds(0, outer - 1)], far_recv.at[b])
        keep_before, forward_before = before[b]
        keep_after, backward_after = after[b]
        shares = [far_in[b, k] for k in range(outer)]
        enter_forward, enter_backward = zero, zero
        for k in range(outer):
            new = shares[k][:tiles] * enter_forward + shares[k][tiles:]
            enter_forward = jnp.where(k < z, new, enter_forward)
        for k in reversed(range(outer)):
            new = shares[k][:tiles] * enter_backward + shares[k][tiles:]
            enter_backward = jnp.where(k > z, new, enter_backward)
        enter_forward = keep_before * enter_forward + forward_before
        enter_backward = keep_after * enter_backward + backward_after
        for t in range(tiles):
            cut = slice(t * LANES, (t + 1) * LANES)
            carried[0, b, :, cut] = enter_forward[t : t + 1]
            carried[1, b, :, cut] = enter_backward[t : t + 1]

    line = width // LANES
    wait(as_sent, sent)

    @pl.when(core == 1)
    def _():
        wait(fade_v.at[pl.ds(0, 2 * batch * tiles * CORES * (outer - 1) // line)], far_sent)


def finish_kernel(base, ahead, behind, enter, out_h, out_v, sem):
    batch, length, _ = base.shape
    copies = []
    for b in range(batch):
        for c in range(CUTS):
            cut = (b, pl.ds(c * (length // CUTS), length // CUTS))
            out_v[cut] = (
                base[cut] + ahead[cut] * enter[0, b] + behind[cut] * enter[1, b]
            ).astype(out_v.dtype)
            copies.append(pltpu.make_async_copy(out_v.at[cut], out_h.at[cut], sem))
            copies[-1].start()
    pltpu.make_async_copy(out_v, out_h, sem).wait()


def finish(base, ahead, behind, enter, kind):
    return pl.pallas_call(
        finish_kernel,
        out_shape=jax.ShapeDtypeStruct(base.shape, kind),
        in_specs=[pl.BlockSpec(memory_space=pltpu.VMEM)] * 4,
        out_specs=pl.BlockSpec(memory_space=pltpu.HBM),
        scratch_shapes=[pltpu.VMEM(base.shape, kind), pltpu.SemaphoreType.DMA],
        compiler_params=pltpu.CompilerParams(vmem_limit_bytes=8 * 2**20),
    )(base, ahead, behind, enter)


def local(outer, total_length, fade_rate, update_in, gate_in):
    batch, length, width = fade_rate.shape
    tiles = width // LANES
    full, f32 = (batch, length, width), jnp.float32
    arguments = (fade_rate, update_in, gate_in)
    base, ahead, behind, enter = pl.pallas_call(
        functools.partial(kernel, outer, total_length),
        out_shape=[jax.ShapeDtypeStruct(full, f32)] * 3
        + [jax.ShapeDtypeStruct((2, batch, 1, width), f32)],
        in_specs=[pl.BlockSpec(memory_space=pltpu.HBM)] * 3,
        out_specs=[pl.BlockSpec(memory_space=pltpu.VMEM)] * 4,
        scratch_shapes=[
            pltpu.VMEM((batch * length, width), f32),
            pltpu.VMEM(full, update_in.dtype),
            pltpu.VMEM(full, gate_in.dtype),
            pltpu.VMEM((ROWS, ROWS), jnp.bfloat16),
            pltpu.VMEM((ROWS, ROWS), jnp.bfloat16),
            pltpu.VMEM(full, f32),
            pltpu.VMEM((batch, length // ROWS, SUB, width), f32),
            pltpu.VMEM((batch, 2 * tiles, LANES), f32),
            pltpu.VMEM((batch, INNER, 2 * tiles, LANES), f32),
            pltpu.VMEM((batch * tiles, LANES), f32),
            pltpu.VMEM((INNER, batch * tiles, LANES), f32),
            pltpu.VMEM((batch, 2, 2 * tiles, LANES), f32),
            pltpu.VMEM((batch, outer, 2 * tiles, LANES), f32),
            pltpu.VMEM((INNER - 1, 3 * batch, tiles, LANES), f32),
            pltpu.SemaphoreType.DMA((batch,)),
            pltpu.SemaphoreType.DMA((batch,)),
            pltpu.SemaphoreType.DMA,
            pltpu.SemaphoreType.DMA((batch,)),
            pltpu.SemaphoreType.DMA,
            pltpu.SemaphoreType.DMA,
            pltpu.SemaphoreType.REGULAR,
        ],
        compiler_params=pltpu.CompilerParams(
            collective_id=0, has_side_effects=True, vmem_limit_bytes=32 * 2**20
        ),
    )(*(pltpu.with_memory_space_constraint(a, pltpu.HBM) for a in arguments))
    return finish(base, ahead, behind, enter, update_in.dtype)


def solution(mesh):
    spec = P(None, "seq", "width")
    devices = mesh.shape["seq"]

    def step(fade_rate, update_in, gate_in):
        body = functools.partial(local, devices // INNER, fade_rate.shape[1])
        return jax.shard_map(
            body, mesh=mesh, in_specs=(spec, spec, spec), out_specs=spec, check_vma=False
        )(fade_rate, update_in, gate_in)

    return step
```

```python
import functools
import math

import jax
import jax.numpy as jnp
from jax import lax
from jax.experimental import pallas as pl
from jax.experimental.pallas import tpu as pltpu
from jax.sharding import PartitionSpec as P

MESH = pl.DeviceIdType.MESH
INNER = 8
CORES = 2
CHIPS = INNER // CORES
LANES = 128
ROWS = 128
SUB = 8
CUTS = 4


def triangle(rows, upper):
    r = lax.broadcasted_iota(jnp.int32, (rows, rows), 0)
    c = lax.broadcasted_iota(jnp.int32, (rows, rows), 1)
    inside = c >= r if upper else c <= r
    return jnp.where(inside, 1.0, 0.0).astype(jnp.bfloat16)


dot = functools.partial(jnp.dot, preferred_element_type=jnp.float32)


def running(mask, value):
    high = value.astype(jnp.bfloat16)
    low = (value - high.astype(jnp.float32)).astype(jnp.bfloat16)
    return dot(mask, high) + dot(mask, low)


def folded(value):
    return jnp.sum(value.reshape(value.shape[0] // SUB, SUB, value.shape[1]), axis=0)


def kernel(
    outer, total_length,
    fade_h, upd_h, gate_h, base, qv, rv, carried,
    fade_v, upd_v, gate_v, lower, upper, logs, into,
    row_out, row_in, last_out, last_in, far_out, far_in, as_sent,
    load_sem, row_recv, last_recv, far_recv, sent, far_sent, told,
):
    batch, length, width = upd_v.shape
    parts = length // ROWS
    tiles = width // LANES
    seq = lax.axis_index("seq")
    z, r = seq // INNER, seq % INNER
    x, core = r // CORES, r % CORES

    def at(row, place):
        return {"seq": row * INNER + place}

    def others(own, count):
        return [k + jnp.where(k >= own, 1, 0) for k in range(count - 1)]

    def signal(sem, peer):
        pl.semaphore_signal(sem, inc=1, device_id=peer, device_id_type=MESH)

    def send(src, dst, out_sem, in_sem, peer):
        pltpu.make_async_remote_copy(
            src_ref=src, dst_ref=dst, send_sem=out_sem, recv_sem=in_sem,
            device_id=peer, device_id_type=MESH,
        ).start()

    def wait(ref, sem):
        pltpu.make_async_copy(ref, ref, sem).wait()

    def load(b):
        half = length // 2
        for h in range(2):
            part = pl.ds(h * half, half)
            to = fade_v.at[pl.ds(b * length + h * half, half)]
            pltpu.make_async_copy(fade_h.at[b, part], to, load_sem.at[b]).start()
            to = upd_v.at[b, part]
            pltpu.make_async_copy(upd_h.at[b, part], to, load_sem.at[b]).start()

    def loaded(b):
        wait(fade_v.at[pl.ds(0, length + length // 2)], load_sem.at[b])

    load(0)
    barrier = pltpu.get_barrier_semaphore()
    for d in range(1, CHIPS):
        signal(barrier, at(z, (x + d) % CHIPS * CORES + 1))

    @pl.when(core == 0)
    def _():
        signal(barrier, at(z, r + 1))

    load(1)
    for row in others(z, outer):
        signal(barrier, at(row, x * CORES))
    lower[...] = triangle(ROWS, False)
    scale = math.log2(math.e) / total_length
    partner = at(z, r + 1 - 2 * core)

    totals, entering = {}, {}

    def summary(b):
        downs = []
        for p in range(parts):
            cut = (b, slice(p * ROWS, (p + 1) * ROWS))
            fade = fade_v[b * length + p * ROWS : b * length + (p + 1) * ROWS] * scale
            log = dot(lower[...], fade.astype(jnp.bfloat16))
            logs[cut] = log
            downs.append(folded(jnp.exp2(fade - log) * upd_v[cut].astype(jnp.float32)))
            totals[b, p] = jnp.sum(folded(fade), axis=0, keepdims=True)
        state = jnp.zeros((SUB, width), jnp.float32)
        for p in reversed(range(parts)):
            entering[b, p] = jnp.exp2(-totals[b, p]) * state
            state = downs[p] + entering[b, p]
            into[b, p] = entering[b, p]
        backward = jnp.sum(state, axis=0, keepdims=True)
        keep = jnp.exp2(-sum(totals[b, p] for p in range(parts)))
        for k, value in enumerate((keep, backward)):
            for t in range(tiles):
                i = k * tiles + t
                row_out[b, i : i + 1, :] = value[:, t * LANES : (t + 1) * LANES]

    def send_row(src, dst, out_sem, in_sem):
        own = (1 - core) * CHIPS + x
        for k in others(own, INNER):
            place = k % CHIPS * CORES + 1 - k // CHIPS
            send(src, dst.at[r], out_sem, in_sem, at(z, place))

    def send_backward(b):
        send_row(row_out.at[b], row_in.at[b], sent, row_recv.at[b])

    loaded(0)
    summary(0)

    @pl.when(core == 1)
    def _():
        pl.semaphore_wait(barrier, INNER - 1)
        signal(told, partner)

    @pl.when(core == 0)
    def _():
        pl.semaphore_wait(told, 1)

    send_backward(0)
    for b in range(1, batch):
        loaded(b)
        summary(b)
        send_backward(b)

    load_gate = pltpu.make_async_copy(gate_h, gate_v, load_sem.at[0])
    load_gate.start()
    upper[...] = triangle(ROWS, True)

    for b in range(batch):
        state = jnp.zeros((1, width), jnp.float32)
        for p in range(parts):
            cut = (b, slice(p * ROWS, (p + 1) * ROWS))
            log = logs[cut]
            push = upd_v[cut].astype(jnp.float32)
            run = running(lower[...], jnp.exp2(log) * push) + state
            state = run[ROWS - 1 :] * jnp.exp2(-totals[b, p])
            base[cut] = run * jnp.exp2(-log)
        for t in range(tiles):
            i = b * tiles + t
            last_out[i : i + 1, :] = state[:, t * LANES : (t + 1) * LANES]
    send_row(last_out, last_in, sent, last_recv)

    @pl.when(core == 0)
    def _():
        pl.semaphore_wait(barrier, CORES * (outer - 1))
        signal(told, partner)

    @pl.when(core == 1)
    def _():
        pl.semaphore_wait(told, 1)

    zero, one = jnp.zeros((tiles, LANES), jnp.float32), jnp.ones((tiles, LANES), jnp.float32)

    def send_far(b, way, row):
        for c in (1, 0):
            send(
                far_out.at[b, way], far_in.at[b, z], far_sent, far_recv.at[b],
                at(row, x * CORES + c),
            )

    before, after = {}, {}
    for b in range(batch):
        row_in[b, pl.ds(r, 1)] = row_out[b][None]
        wait(row_in.at[b, pl.ds(0, INNER - 1)], row_recv.at[b])
        shares = [row_in[b, k] for k in range(INNER)]
        keep_row, backward_row, keep_after, backward_after = one, zero, one, zero
        for k in reversed(range(INNER)):
            backward_row = shares[k][:tiles] * backward_row + shares[k][tiles:]
            keep_row = shares[k][:tiles] * keep_row
            keep_after = jnp.where(k > r, keep_row, keep_after)
            backward_after = jnp.where(k > r, backward_row, backward_after)
        after[b] = keep_after, backward_after
        far_out[b, 0, :tiles] = keep_row
        far_out[b, 1, :tiles] = keep_row
        far_out[b, 1, tiles:] = backward_row
        for row in range(outer - 1):

            @pl.when((core == 1) & (row < z))
            def _():
                send_far(b, 1, row)

    last_in[pl.ds(r, 1)] = last_out[...][None]
    wait(last_in.at[pl.ds(0, INNER - 1)], last_recv)
    for b in range(batch):
        keep_row, forward_row, keep_before, forward_before = one, zero, one, zero
        for k in range(INNER):
            keep = row_in[b, k, :tiles]
            forward_row = keep * forward_row + last_in[k, b * tiles : (b + 1) * tiles]
            keep_row = keep * keep_row
            keep_before = jnp.where(k < r, keep_row, keep_before)
            forward_before = jnp.where(k < r, forward_row, forward_before)
        before[b] = keep_before, forward_before
        far_out[b, 0, tiles:] = forward_row
        for row in range(1, outer):

            @pl.when((core == 1) & (row > z))
            def _():
                send_far(b, 0, row)

    load_gate.wait()
    for b in range(batch):
        passed = jnp.zeros((1, width), jnp.float32)
        for p in range(parts):
            cut = (b, slice(p * ROWS, (p + 1) * ROWS))
            log = logs[cut]
            short = log - fade_v[b * length + p * ROWS : b * length + (p + 1) * ROWS] * scale
            push = upd_v[cut].astype(jnp.float32)
            enter = jnp.sum(into[b, p], axis=0, keepdims=True)
            run = running(upper[...], jnp.exp2(-short) * push) + enter
            gate = gate_v[cut].astype(jnp.float32)
            gate = gate * (total_length**-0.5) / (1.0 + jnp.exp(-gate))
            raised = jnp.exp2(short) * gate
            base[cut] = base[cut] * gate + run * raised
            left = sum(totals[b, q] for q in range(p, parts))
            qv[cut] = jnp.exp2(-log) * gate * jnp.exp2(-passed)
            rv[cut] = raised * jnp.exp2(-left)
            passed = passed + totals[b, p]

    for b in range(batch):
        far_in[b, pl.ds(z, 1)] = far_out[b, 0:1]
        wait(far_in.at[b, pl.ds(0, outer - 1)], far_recv.at[b])
        keep_before, forward_before = before[b]
        keep_after, backward_after = after[b]
        shares = [far_in[b, k] for k in range(outer)]
        enter_forward, enter_backward = zero, zero
        for k in range(outer):
            new = shares[k][:tiles] * enter_forward + shares[k][tiles:]
            enter_forward = jnp.where(k < z, new, enter_forward)
        for k in reversed(range(outer)):
            new = shares[k][:tiles] * enter_backward + shares[k][tiles:]
            enter_backward = jnp.where(k > z, new, enter_backward)
        enter_forward = keep_before * enter_forward + forward_before
        enter_backward = keep_after * enter_backward + backward_after
        for t in range(tiles):
            cut = slice(t * LANES, (t + 1) * LANES)
            carried[0, b, :, cut] = enter_forward[t : t + 1]
            carried[1, b, :, cut] = enter_backward[t : t + 1]

    line = width // LANES
    wait(as_sent, sent)

    @pl.when(core == 1)
    def _():
        wait(fade_v.at[pl.ds(0, 2 * batch * tiles * CORES * (outer - 1) // line)], far_sent)


def finish_kernel(base, ahead, behind, enter, out_h, out_v, sem):
    batch, length, _ = base.shape
    copies = []
    for b in range(batch):
        for c in range(CUTS):
            cut = (b, pl.ds(c * (length // CUTS), length // CUTS))
            out_v[cut] = (
                base[cut] + ahead[cut] * enter[0, b] + behind[cut] * enter[1, b]
            ).astype(out_v.dtype)
            copies.append(pltpu.make_async_copy(out_v.at[cut], out_h.at[cut], sem))
            copies[-1].start()
    pltpu.make_async_copy(out_v, out_h, sem).wait()


def finish(base, ahead, behind, enter, kind):
    return pl.pallas_call(
        finish_kernel,
        out_shape=jax.ShapeDtypeStruct(base.shape, kind),
        in_specs=[pl.BlockSpec(memory_space=pltpu.VMEM)] * 4,
        out_specs=pl.BlockSpec(memory_space=pltpu.HBM),
        scratch_shapes=[pltpu.VMEM(base.shape, kind), pltpu.SemaphoreType.DMA],
        compiler_params=pltpu.CompilerParams(vmem_limit_bytes=8 * 2**20),
    )(base, ahead, behind, enter)


def local(outer, total_length, fade_rate, update_in, gate_in):
    batch, length, width = fade_rate.shape
    tiles = width // LANES
    full, f32 = (batch, length, width), jnp.float32
    arguments = (fade_rate, update_in, gate_in)
    base, ahead, behind, enter = pl.pallas_call(
        functools.partial(kernel, outer, total_length),
        out_shape=[jax.ShapeDtypeStruct(full, f32)] * 3
        + [jax.ShapeDtypeStruct((2, batch, 1, width), f32)],
        in_specs=[pl.BlockSpec(memory_space=pltpu.HBM)] * 3,
        out_specs=[pl.BlockSpec(memory_space=pltpu.VMEM)] * 4,
        scratch_shapes=[
            pltpu.VMEM((batch * length, width), f32),
            pltpu.VMEM(full, update_in.dtype),
            pltpu.VMEM(full, gate_in.dtype),
            pltpu.VMEM((ROWS, ROWS), jnp.bfloat16),
            pltpu.VMEM((ROWS, ROWS), jnp.bfloat16),
            pltpu.VMEM(full, f32),
            pltpu.VMEM((batch, length // ROWS, SUB, width), f32),
            pltpu.VMEM((batch, 2 * tiles, LANES), f32),
            pltpu.VMEM((batch, INNER, 2 * tiles, LANES), f32),
            pltpu.VMEM((batch * tiles, LANES), f32),
            pltpu.VMEM((INNER, batch * tiles, LANES), f32),
            pltpu.VMEM((batch, 2, 2 * tiles, LANES), f32),
            pltpu.VMEM((batch, outer, 2 * tiles, LANES), f32),
            pltpu.VMEM((INNER - 1, 3 * batch, tiles, LANES), f32),
            pltpu.SemaphoreType.DMA((batch,)),
            pltpu.SemaphoreType.DMA((batch,)),
            pltpu.SemaphoreType.DMA,
            pltpu.SemaphoreType.DMA((batch,)),
            pltpu.SemaphoreType.DMA,
            pltpu.SemaphoreType.DMA,
            pltpu.SemaphoreType.REGULAR,
        ],
        compiler_params=pltpu.CompilerParams(
            collective_id=0, has_side_effects=True, vmem_limit_bytes=32 * 2**20
        ),
    )(*(pltpu.with_memory_space_constraint(a, pltpu.HBM) for a in arguments))
    return finish(base, ahead, behind, enter, update_in.dtype)


def solution(mesh):
    spec = P(None, "seq", "width")
    devices = mesh.shape["seq"]

    def step(fade_rate, update_in, gate_in):
        body = functools.partial(local, devices // INNER, fade_rate.shape[1])
        return jax.shard_map(
            body, mesh=mesh, in_specs=(spec, spec, spec), out_specs=spec, check_vma=False
        )(fade_rate, update_in, gate_in)

    return step
```

```python
import functools
import math

import jax
import jax.numpy as jnp
from jax import lax
from jax.experimental import pallas as pl
from jax.experimental.pallas import tpu as pltpu
from jax.sharding import PartitionSpec as P

MESH = pl.DeviceIdType.MESH
INNER = 8
CORES = 2
CHIPS = INNER // CORES
LANES = 128
ROWS = 128
SUB = 8
CUTS = 4


def triangle(rows, upper):
    r = lax.broadcasted_iota(jnp.int32, (rows, rows), 0)
    c = lax.broadcasted_iota(jnp.int32, (rows, rows), 1)
    inside = c >= r if upper else c <= r
    return jnp.where(inside, 1.0, 0.0).astype(jnp.bfloat16)


dot = functools.partial(jnp.dot, preferred_element_type=jnp.float32)


def running(mask, value):
    high = value.astype(jnp.bfloat16)
    low = (value - high.astype(jnp.float32)).astype(jnp.bfloat16)
    return dot(mask, high) + dot(mask, low)


def folded(value):
    return jnp.sum(value.reshape(value.shape[0] // SUB, SUB, value.shape[1]), axis=0)


def joined(pairs):
    while len(pairs) > 1:
        ends = [(p[0] * q[0], p[1] + p[0] * q[1]) for p, q in zip(pairs[::2], pairs[1::2])]
        pairs = ends + pairs[len(pairs) // 2 * 2 :]
    return pairs[0][1]


def kernel(
    outer, total_length,
    fade_h, upd_h, gate_h, base, qv, rv, carried,
    fade_v, upd_v, gate_v, lower, upper, logs, into,
    row_out, row_in, last_out, last_in, far_out, far_in, as_sent,
    load_sem, row_recv, last_recv, far_recv, sent, far_sent, told,
):
    batch, length, width = upd_v.shape
    parts = length // ROWS
    tiles = width // LANES
    seq = lax.axis_index("seq")
    z, r = seq // INNER, seq % INNER
    x, core = r // CORES, r % CORES

    def at(row, place):
        return {"seq": row * INNER + place}

    def others(own, count):
        return [k + jnp.where(k >= own, 1, 0) for k in range(count - 1)]

    def signal(sem, peer):
        pl.semaphore_signal(sem, inc=1, device_id=peer, device_id_type=MESH)

    def send(src, dst, out_sem, in_sem, peer):
        pltpu.make_async_remote_copy(
            src_ref=src, dst_ref=dst, send_sem=out_sem, recv_sem=in_sem,
            device_id=peer, device_id_type=MESH,
        ).start()

    def wait(ref, sem):
        pltpu.make_async_copy(ref, ref, sem).wait()

    def load(b):
        half = length // 2
        for h in range(2):
            part = pl.ds(h * half, half)
            to = fade_v.at[pl.ds(b * length + h * half, half)]
            pltpu.make_async_copy(fade_h.at[b, part], to, load_sem.at[b]).start()
            to = upd_v.at[b, part]
            pltpu.make_async_copy(upd_h.at[b, part], to, load_sem.at[b]).start()

    def loaded(b):
        wait(fade_v.at[pl.ds(0, length + length // 2)], load_sem.at[b])

    load(0)
    barrier = pltpu.get_barrier_semaphore()
    for d in range(1, CHIPS):
        signal(barrier, at(z, (x + d) % CHIPS * CORES + 1))

    @pl.when(core == 0)
    def _():
        signal(barrier, at(z, r + 1))

    load(1)
    for row in others(z, outer):
        signal(barrier, at(row, x * CORES))
    lower[...] = triangle(ROWS, False)
    scale = math.log2(math.e) / total_length
    partner = at(z, r + 1 - 2 * core)

    totals, entering = {}, {}

    def summary(b):
        downs = []
        for p in range(parts):
            cut = (b, slice(p * ROWS, (p + 1) * ROWS))
            fade = fade_v[b * length + p * ROWS : b * length + (p + 1) * ROWS] * scale
            log = dot(lower[...], fade.astype(jnp.bfloat16))
            logs[cut] = log
            downs.append(folded(jnp.exp2(fade - log) * upd_v[cut].astype(jnp.float32)))
            totals[b, p] = jnp.sum(folded(fade), axis=0, keepdims=True)
        state = jnp.zeros((SUB, width), jnp.float32)
        for p in reversed(range(parts)):
            entering[b, p] = jnp.exp2(-totals[b, p]) * state
            state = downs[p] + entering[b, p]
            into[b, p] = entering[b, p]
        backward = jnp.sum(state, axis=0, keepdims=True)
        keep = jnp.exp2(-sum(totals[b, p] for p in range(parts)))
        for k, value in enumerate((keep, backward)):
            for t in range(tiles):
                i = k * tiles + t
                row_out[b, i : i + 1, :] = value[:, t * LANES : (t + 1) * LANES]

    def send_row(src, dst, out_sem, in_sem):
        own = (1 - core) * CHIPS + x
        for k in others(own, INNER):
            place = k % CHIPS * CORES + 1 - k // CHIPS
            send(src, dst.at[r], out_sem, in_sem, at(z, place))

    def send_backward(b):
        send_row(row_out.at[b], row_in.at[b], sent, row_recv.at[b])

    loaded(0)
    summary(0)

    @pl.when(core == 1)
    def _():
        pl.semaphore_wait(barrier, INNER - 1)
        signal(told, partner)

    @pl.when(core == 0)
    def _():
        pl.semaphore_wait(told, 1)

    send_backward(0)
    for b in range(1, batch):
        loaded(b)
        summary(b)
        send_backward(b)

    load_gate = pltpu.make_async_copy(gate_h, gate_v, load_sem.at[0])
    load_gate.start()
    upper[...] = triangle(ROWS, True)

    for b in range(batch):
        state = jnp.zeros((1, width), jnp.float32)
        for p in range(parts):
            cut = (b, slice(p * ROWS, (p + 1) * ROWS))
            log = logs[cut]
            push = upd_v[cut].astype(jnp.float32)
            run = running(lower[...], jnp.exp2(log) * push) + state
            state = run[ROWS - 1 :] * jnp.exp2(-totals[b, p])
            base[cut] = run * jnp.exp2(-log)
        for t in range(tiles):
            i = b * tiles + t
            last_out[i : i + 1, :] = state[:, t * LANES : (t + 1) * LANES]
    send_row(last_out, last_in, sent, last_recv)

    @pl.when(core == 0)
    def _():
        pl.semaphore_wait(barrier, CORES * (outer - 1))
        signal(told, partner)

    @pl.when(core == 1)
    def _():
        pl.semaphore_wait(told, 1)

    zero, one = jnp.zeros((tiles, LANES), jnp.float32), jnp.ones((tiles, LANES), jnp.float32)

    def send_far(b, way, row):
        for c in (1, 0):
            send(
                far_out.at[b, way], far_in.at[b, z], far_sent, far_recv.at[b],
                at(row, x * CORES + c),
            )

    before, after = {}, {}
    for b in range(batch):
        row_in[b, pl.ds(r, 1)] = row_out[b][None]
        wait(row_in.at[b, pl.ds(0, INNER - 1)], row_recv.at[b])
        shares = [row_in[b, k] for k in range(INNER)]
        keep_row, backward_row, keep_after, backward_after = one, zero, one, zero
        for k in reversed(range(INNER)):
            backward_row = shares[k][:tiles] * backward_row + shares[k][tiles:]
            keep_row = shares[k][:tiles] * keep_row
            keep_after = jnp.where(k > r, keep_row, keep_after)
            backward_after = jnp.where(k > r, backward_row, backward_after)
        after[b] = keep_after, backward_after
        far_out[b, 0, :tiles] = keep_row
        far_out[b, 1, :tiles] = keep_row
        far_out[b, 1, tiles:] = backward_row
        for row in range(outer - 1):

            @pl.when((core == 1) & (row < z))
            def _():
                send_far(b, 1, row)

    last_in[pl.ds(r, 1)] = last_out[...][None]
    wait(last_in.at[pl.ds(0, INNER - 1)], last_recv)
    for b in range(batch):
        keep_row, forward_row, keep_before, forward_before = one, zero, one, zero
        for k in range(INNER):
            keep = row_in[b, k, :tiles]
            forward_row = keep * forward_row + last_in[k, b * tiles : (b + 1) * tiles]
            keep_row = keep * keep_row
            keep_before = jnp.where(k < r, keep_row, keep_before)
            forward_before = jnp.where(k < r, forward_row, forward_before)
        before[b] = keep_before, forward_before
        far_out[b, 0, tiles:] = forward_row
        for row in range(1, outer):

            @pl.when((core == 1) & (row > z))
            def _():
                send_far(b, 0, row)

    load_gate.wait()
    for b in range(batch):
        passed = jnp.zeros((1, width), jnp.float32)
        for p in range(parts):
            cut = (b, slice(p * ROWS, (p + 1) * ROWS))
            log = logs[cut]
            short = log - fade_v[b * length + p * ROWS : b * length + (p + 1) * ROWS] * scale
            push = upd_v[cut].astype(jnp.float32)
            enter = jnp.sum(into[b, p], axis=0, keepdims=True)
            run = running(upper[...], jnp.exp2(-short) * push) + enter
            gate = gate_v[cut].astype(jnp.float32)
            gate = gate * (total_length**-0.5) / (1.0 + jnp.exp(-gate))
            raised = jnp.exp2(short) * gate
            base[cut] = base[cut] * gate + run * raised
            left = sum(totals[b, q] for q in range(p, parts))
            qv[cut] = jnp.exp2(-log) * gate * jnp.exp2(-passed)
            rv[cut] = raised * jnp.exp2(-left)
            passed = passed + totals[b, p]

    for b in range(batch):
        far_in[b, pl.ds(z, 1)] = far_out[b, 0:1]
        wait(far_in.at[b, pl.ds(0, outer - 1)], far_recv.at[b])
        keep_before, forward_before = before[b]
        keep_after, backward_after = after[b]
        shares = [(far_in[b, k, :tiles], far_in[b, k, tiles:]) for k in range(outer)]

        def taken(k, wanted):
            return tuple(jnp.where(wanted, v, e) for v, e in zip(shares[k], (one, zero)))

        enter_forward = joined([taken(k, k < z) for k in reversed(range(outer))])
        enter_backward = joined([taken(k, k > z) for k in range(outer)])
        enter_forward = keep_before * enter_forward + forward_before
        enter_backward = keep_after * enter_backward + backward_after
        for t in range(tiles):
            cut = slice(t * LANES, (t + 1) * LANES)
            carried[0, b, :, cut] = enter_forward[t : t + 1]
            carried[1, b, :, cut] = enter_backward[t : t + 1]

    line = width // LANES
    wait(as_sent, sent)

    @pl.when(core == 1)
    def _():
        wait(fade_v.at[pl.ds(0, 2 * batch * tiles * CORES * (outer - 1) // line)], far_sent)


def finish_kernel(base, ahead, behind, enter, out_h, out_v, sem):
    batch, length, _ = base.shape
    copies = []
    for b in range(batch):
        for c in range(CUTS):
            cut = (b, pl.ds(c * (length // CUTS), length // CUTS))
            out_v[cut] = (
                base[cut] + ahead[cut] * enter[0, b] + behind[cut] * enter[1, b]
            ).astype(out_v.dtype)
            copies.append(pltpu.make_async_copy(out_v.at[cut], out_h.at[cut], sem))
            copies[-1].start()
    pltpu.make_async_copy(out_v, out_h, sem).wait()


def finish(base, ahead, behind, enter, kind):
    return pl.pallas_call(
        finish_kernel,
        out_shape=jax.ShapeDtypeStruct(base.shape, kind),
        in_specs=[pl.BlockSpec(memory_space=pltpu.VMEM)] * 4,
        out_specs=pl.BlockSpec(memory_space=pltpu.HBM),
        scratch_shapes=[pltpu.VMEM(base.shape, kind), pltpu.SemaphoreType.DMA],
        compiler_params=pltpu.CompilerParams(vmem_limit_bytes=8 * 2**20),
    )(base, ahead, behind, enter)


def local(outer, total_length, fade_rate, update_in, gate_in):
    batch, length, width = fade_rate.shape
    tiles = width // LANES
    full, f32 = (batch, length, width), jnp.float32
    arguments = (fade_rate, update_in, gate_in)
    base, ahead, behind, enter = pl.pallas_call(
        functools.partial(kernel, outer, total_length),
        out_shape=[jax.ShapeDtypeStruct(full, f32)] * 3
        + [jax.ShapeDtypeStruct((2, batch, 1, width), f32)],
        in_specs=[pl.BlockSpec(memory_space=pltpu.HBM)] * 3,
        out_specs=[pl.BlockSpec(memory_space=pltpu.VMEM)] * 4,
        scratch_shapes=[
            pltpu.VMEM((batch * length, width), f32),
            pltpu.VMEM(full, update_in.dtype),
            pltpu.VMEM(full, gate_in.dtype),
            pltpu.VMEM((ROWS, ROWS), jnp.bfloat16),
            pltpu.VMEM((ROWS, ROWS), jnp.bfloat16),
            pltpu.VMEM(full, f32),
            pltpu.VMEM((batch, length // ROWS, SUB, width), f32),
            pltpu.VMEM((batch, 2 * tiles, LANES), f32),
            pltpu.VMEM((batch, INNER, 2 * tiles, LANES), f32),
            pltpu.VMEM((batch * tiles, LANES), f32),
            pltpu.VMEM((INNER, batch * tiles, LANES), f32),
            pltpu.VMEM((batch, 2, 2 * tiles, LANES), f32),
            pltpu.VMEM((batch, outer, 2 * tiles, LANES), f32),
            pltpu.VMEM((INNER - 1, 3 * batch, tiles, LANES), f32),
            pltpu.SemaphoreType.DMA((batch,)),
            pltpu.SemaphoreType.DMA((batch,)),
            pltpu.SemaphoreType.DMA,
            pltpu.SemaphoreType.DMA((batch,)),
            pltpu.SemaphoreType.DMA,
            pltpu.SemaphoreType.DMA,
            pltpu.SemaphoreType.REGULAR,
        ],
        compiler_params=pltpu.CompilerParams(
            collective_id=0, has_side_effects=True, vmem_limit_bytes=32 * 2**20
        ),
    )(*(pltpu.with_memory_space_constraint(a, pltpu.HBM) for a in arguments))
    return finish(base, ahead, behind, enter, update_in.dtype)


def solution(mesh):
    spec = P(None, "seq", "width")
    devices = mesh.shape["seq"]

    def step(fade_rate, update_in, gate_in):
        body = functools.partial(local, devices // INNER, fade_rate.shape[1])
        return jax.shard_map(
            body, mesh=mesh, in_specs=(spec, spec, spec), out_specs=spec, check_vma=False
        )(fade_rate, update_in, gate_in)

    return step
```
